16 devices in a mesh: dp: 1, tp: 16 (over x, y, z, core).
Axes of the slice: x: 2, y: 2, z: 2, core: 2. Of those that a mesh axis runs over, the one named last changes fastest.
Arguments:
- x: bfloat16 [2560, 7168], P(('dp', 'tp'))
- dy: bfloat16 [2560, 7168], P(('dp', 'tp'))
- gate: bfloat16 [2560, 18432], P('dp', 'tp')
- up: bfloat16 [2560, 18432], P('dp', 'tp')
- w_gate: bfloat16 [7168, 18432], P(None, 'tp')
- w_up: bfloat16 [7168, 18432], P(None, 'tp')
- w_down: bfloat16 [18432, 7168], P('tp')
Outputs:
- output 1: bfloat16 [2560, 7168], P(('dp', 'tp'))
- output 2: bfloat16 [7168, 18432], P('dp', 'tp')
- output 3: bfloat16 [7168, 18432], P('dp', 'tp')
- output 4: bfloat16 [18432, 7168], P(('dp', 'tp'))
All inputs are finite; a program needn't handle non-finite values.
Results may differ from the reference program's by a relative error of at most 0.012.
Values are sent between devices in bfloat16 or wider.
A program may use at most 2 GiB of HBM per device.

```python
import jax
import jax.numpy as jnp

ROWS = 2560
D = 7168
FF = 18432


def act(gate, up):
    return jax.nn.silu(gate) * up


def setup_inputs(seed: int = 0, part: int = 0) -> dict:
    kx, ky, ka, kb, kg, ku, kd = jax.random.split(jax.random.key(seed), 7)
    kx, ky, ka, kb = (jax.random.fold_in(k, part) for k in (kx, ky, ka, kb))
    drawn = {
        "x": jax.random.normal(kx, (ROWS, D), jnp.float32),
        "dy": jax.random.normal(ky, (ROWS, D), jnp.float32),
        "gate": jax.random.normal(ka, (ROWS, FF), jnp.float32),
        "up": jax.random.normal(kb, (ROWS, FF), jnp.float32),
        "w_gate": jax.random.normal(kg, (D, FF), jnp.float32) * D**-0.5,
        "w_up": jax.random.normal(ku, (D, FF), jnp.float32) * D**-0.5,
        "w_down": jax.random.normal(kd, (FF, D), jnp.float32) * FF**-0.5,
    }
    return {k: v.astype(jnp.bfloat16) for k, v in drawn.items()}


def reference(x, dy, gate, up, w_gate, w_up, w_down):
    hidden, back = jax.vjp(act, gate.astype(jnp.float32), up.astype(jnp.float32))
    d_hidden = jnp.dot(dy, w_down.T, preferred_element_type=jnp.float32)
    d_gate, d_up = (g.astype(jnp.bfloat16) for g in back(d_hidden))
    dx = jnp.dot(d_gate, w_gate.T, preferred_element_type=jnp.float32) + jnp.dot(d_up, w_up.T, preferred_element_type=jnp.float32)
    dw_gate = jnp.dot(x.T, d_gate, preferred_element_type=jnp.float32)
    dw_up = jnp.dot(x.T, d_up, preferred_element_type=jnp.float32)
    dw_down = jnp.dot(hidden.astype(jnp.bfloat16).T, dy, preferred_element_type=jnp.float32)
    return tuple(g.astype(jnp.bfloat16) for g in (dx, dw_gate, dw_up, dw_down))
```

```python
import jax
import jax.numpy as jnp
from jax import lax
from jax.experimental import pallas as pl
from jax.experimental.pallas import tpu as pltpu
from jax.sharding import PartitionSpec as P

ROWS, D, FF, N = 2560, 7168, 18432, 16
SHARD, F = ROWS // N, FF // N
C = 512
CHUNKS = D // C
PIECES = ((0, 56), (56, 56), (112, 48))
T = 256
TILES = ROWS // T
E = 256
STEPS = D // E
LAG_B, LAG_C, LAG_D, LAG_E = 1, 3, 5, 7
BF, F32 = jnp.bfloat16, jnp.float32
NT = (((1,), (1,)), ((), ()))
TN = (((0,), (0,)), ((), ()))
ANY = pl.BlockSpec(memory_space=pl.ANY)


def dot(a, b, dims=(((1,), (0,)), ((), ()))):
    return lax.dot_general(a, b, dims, preferred_element_type=F32)


def across(device, mask):
    return device + mask * (1 - 2 * lax.rem(lax.div(device, jnp.int32(mask)), jnp.int32(2)))


def axis_mask(i):
    return 8 - 5 * i + i * i


def masks(start):
    i = [lax.rem(jnp.int32(start + k), jnp.int32(3)) for k in range(3)]
    return [axis_mask(k) for k in i]


def loop(lo, hi, body):
    lax.fori_loop(lo, hi, lambda i, c: (body(i), c)[1], 0)


class Gather:
    SEMS = [
        pltpu.SemaphoreType.DMA((3, 3 * CHUNKS)),
        pltpu.SemaphoreType.DMA((CHUNKS,)),
        pltpu.SemaphoreType.DMA((CHUNKS,)),
        pltpu.SemaphoreType.DMA((2,)),
    ]

    def __init__(self, own, g, buf, arrived, paired, sent, loaded):
        self.own_ref, self.g, self.buf = own, g, buf
        self.arrived, self.paired, self.sent, self.loaded = arrived, paired, sent, loaded
        self.me = lax.axis_index("tp").astype(jnp.int32)

    def cols(self, j):
        return pl.ds(pl.multiple_of(j * C, C), C)

    def send(self, j, q, shard, to, phase, src=None):
        rows = pl.ds(*PIECES[q])
        place = self.g.at[shard, rows, self.cols(j)]
        src = place if src is None else src.at[rows, self.cols(j)]
        sem = self.paired.at[j] if phase == 3 else self.arrived.at[phase, 3 * j + q]
        pltpu.make_async_remote_copy(
            src, place, self.sent.at[j], sem, device_id={"tp": to}, device_id_type=pl.DeviceIdType.MESH
        ).start()

    def wait(self, sem, shards, rows):
        ref = self.g.at[pl.ds(0, shards), pl.ds(0, rows), pl.ds(0, C)]
        pltpu.make_async_copy(ref, ref, sem).wait()

    def first(self, j):
        for q in range(3):
            m = masks(j + q)
            for phase in range(3):
                self.send(j, q, self.me, across(self.me, m[phase]), phase, self.own_ref)
            self.send(j, q, self.me, across(self.me, 1), 3, self.own_ref)

    def forward(self, phase, j):
        for q in range(3):
            self.wait(self.arrived.at[phase, 3 * j + q], 2**phase, PIECES[q][1])
            m = masks(j + q)
            shards = [across(self.me, m[phase])]
            for earlier in range(phase):
                shards += [across(s, m[earlier]) for s in shards]
            for s in shards:
                for later in range(phase + 1, 3):
                    self.send(j, q, s, across(self.me, m[later]), later)
                self.send(j, q, s, across(self.me, 1), 3)

    def load(self, j):
        self.wait(self.paired.at[j], 8, SHARD)
        slot = lax.rem(j, 2)
        for r in range(N):
            s = lax.rem(self.me + r, N)
            src = self.own_ref.at[:, self.cols(j)] if r == 0 else self.g.at[s, :, self.cols(j)]
            dst = self.buf.at[slot, pl.ds(pl.multiple_of(s * SHARD, SHARD), SHARD)]
            pltpu.make_async_copy(src, dst, self.loaded.at[slot]).start()

    def pump(self, t):
        def at(lead, f):
            j = t + lead

            @pl.when((j >= 0) & (j < CHUNKS))
            def _():
                f(j)

        at(1, self.load)
        at(2, lambda j: self.forward(2, j))
        at(3, lambda j: self.forward(1, j))
        at(4, lambda j: self.forward(0, j))
        at(7, self.first)

    def start(self):
        for j in range(3):
            self.first(jnp.int32(j))

    def held(self, j):
        slot = lax.rem(j, 2)
        ref = self.buf.at[slot]
        pltpu.make_async_copy(ref, ref, self.loaded.at[slot]).wait()
        return slot

    def finish(self):
        loop(0, CHUNKS, lambda j: self.wait(self.sent.at[j], 15, SHARD))


def wait_like(ref, sem):
    pltpu.make_async_copy(ref, ref, sem).wait()


def hidden_kernel(dy, gate, up, w_down, g, d_out, dw_out, acc, ht, buf, w, o, kept, d, *sems):
    *gs, w_sem, o_sem, kept_sem, d_sem = sems
    ag = Gather(dy, g, buf, *gs)
    ag.start()

    def fetch(i):
        slot = lax.rem(i, 2)
        rows = pl.ds(pl.multiple_of(i * T, T), T)
        pltpu.make_async_copy(gate.at[rows], kept.at[slot, 0], kept_sem.at[slot]).start()
        pltpu.make_async_copy(up.at[rows], kept.at[slot, 1], kept_sem.at[slot]).start()

    def tile(i):
        @pl.when(i + 1 < TILES)
        def _():
            fetch(i + 1)

        slot = lax.rem(i, 2)
        wait_like(kept.at[slot], kept_sem.at[slot])
        return slot, pl.ds(pl.multiple_of(i * T, T), T)

    def w_fetch(j):
        slot = lax.rem(j, 2)
        pltpu.make_async_copy(w_down.at[:, ag.cols(j)], w.at[slot], w_sem.at[slot]).start()

    fetch(jnp.int32(0))
    w_fetch(jnp.int32(0))

    def hide(i):
        slot, rows = tile(i)
        gt, ut = kept[slot, 0].astype(F32), kept[slot, 1].astype(F32)
        h = gt * jax.nn.sigmoid(gt) * ut
        ht[:, rows] = h.T.astype(BF)
        acc[rows, :] = jnp.zeros((T, F), F32)

        @pl.when((lax.rem(i, 2) == 1) & (i < 8))
        def _():
            ag.pump(lax.div(i, 2) - 4)

    loop(0, TILES, hide)

    def chunk(j):
        ag.pump(j)

        @pl.when(j + 1 < CHUNKS)
        def _():
            w_fetch(j + 1)

        slot = ag.held(j)
        wait_like(w.at[slot], w_sem.at[slot])

        def rows_of(i):
            rows = pl.ds(pl.multiple_of(i * T, T), T)
            acc[rows, :] += dot(buf[slot, rows, :], w[slot], NT)

        loop(0, TILES, rows_of)

        @pl.when(j >= 2)
        def _():
            wait_like(o.at[slot], o_sem.at[slot])

        def columns_of(i):
            rows = pl.ds(pl.multiple_of(i * 384, 384), 384)
            o[slot, rows, :] = dot(ht[rows, :], buf[slot]).astype(BF)

        loop(0, F // 384, columns_of)
        pltpu.make_async_copy(o.at[slot], dw_out.at[:, ag.cols(j)], o_sem.at[slot]).start()

    loop(0, CHUNKS, chunk)
    fetch(jnp.int32(0))

    def back(i):
        slot, rows = tile(i)

        @pl.when(i >= 2)
        def _():
            wait_like(d.at[slot], d_sem.at[slot])

        gt, ut, dh = kept[slot, 0].astype(F32), kept[slot, 1].astype(F32), acc[rows, :]
        s = jax.nn.sigmoid(gt)
        d[slot, :, :F] = (dh * ut * (s * (1 + gt * (1 - s)))).astype(BF)
        d[slot, :, F:] = (dh * (gt * s)).astype(BF)
        pltpu.make_async_copy(d.at[slot], d_out.at[rows], d_sem.at[slot]).start()

    loop(0, TILES, back)
    for slot in range(2):
        wait_like(d.at[slot], d_sem.at[slot])
        wait_like(o.at[slot], o_sem.at[slot])
    ag.finish()


def weights_kernel(x, d_in, g, dwg, dwu, buf, d, o, *sems):
    *gs, d_sem, o_sem = sems
    ag = Gather(x, g, buf, *gs)
    ag.start()
    pltpu.make_async_copy(d_in, d, d_sem).start()
    loop(-4, 0, ag.pump)
    wait_like(d, d_sem)

    def chunk(j):
        ag.pump(j)
        slot = ag.held(j)

        @pl.when(j >= 2)
        def _():
            wait_like(o.at[slot], o_sem.at[slot])

        for half in range(2):
            for i in range(C // 256):
                cols = pl.ds(i * 256, 256)
                o[slot, half, cols, :] = dot(buf[slot, :, cols], d[:, pl.ds(half * F, F)], TN).astype(BF)
        rows = pl.ds(pl.multiple_of(j * C, C), C)
        pltpu.make_async_copy(o.at[slot, 0], dwg.at[rows], o_sem.at[slot]).start()
        pltpu.make_async_copy(o.at[slot, 1], dwu.at[rows], o_sem.at[slot]).start()

    loop(0, CHUNKS, chunk)
    for slot in range(2):
        wait_like(o.at[slot], o_sem.at[slot])
    ag.finish()


def sum_kernel(d_in, w_gate, w_up, dx, pair, l1, l2, l3, w, d, sa, sb, sc, sd, se, ab, ac, ad, ae, *sems):
    d_sem, w_sem, pair_sem, r1, r2, r3, send_sem, load_sem, out_sem = sems
    me = lax.axis_index("tp").astype(jnp.int32)
    partner = across(me, 1)
    for half in range(2):
        for r in range(8):
            device = across(me, 1) if half else me
            for bit in (1, 2, 4):
                if r & bit:
                    device = across(device, 2 * bit)
            src = d_in.at[pl.ds(pl.multiple_of(device * SHARD, SHARD), SHARD)]
            pltpu.make_async_copy(src, d.at[pl.ds((half * 8 + r) * SHARD, SHARD)], d_sem).start()

    def w_copies(t):
        rows = pl.ds(pl.multiple_of(t * E, E), E)
        return [
            pltpu.make_async_copy(w_gate.at[rows], w.at[rows, pl.ds(0, F)], w_sem.at[0, t]),
            pltpu.make_async_copy(w_up.at[rows], w.at[rows, pl.ds(F, F)], w_sem.at[1, t]),
        ]

    def w_start(t):
        for c in w_copies(t):
            c.start()

    loop(0, STEPS, w_start)
    wait_like(d, d_sem)

    def part(t, block, blocks=1):
        rows = pl.ds(pl.multiple_of(block * SHARD, SHARD), blocks * SHARD)
        return dot(d[rows, :], w[pl.ds(pl.multiple_of(t * E, E), E), :], NT)

    def send(stage, src, dst, recv, to, slot):
        pltpu.make_async_remote_copy(
            src, dst, send_sem.at[stage, slot], recv, device_id={"tp": to}, device_id_type=pl.DeviceIdType.MESH
        ).start()

    def step(t):
        def at(lag, f):
            u = t - lag

            @pl.when((u >= 0) & (u < STEPS))
            def _():
                m = masks(u)
                f(u, m, [lax.div(k, 2) for k in m])

        def fetch(stage, srcs, buf):
            for k, s in enumerate(srcs):
                pltpu.make_async_copy(s, buf.at[k], load_sem.at[stage]).start()

        def fetch_b(u, m, r):
            wait_like(pair.at[u], pair_sem.at[u])
            fetch(0, [pair.at[u, r[0] + i * r[1] + k * r[2]] for i in range(2) for k in range(2)], ab)

        def fetch_c(u, m, r):
            wait_like(l1.at[u], r1.at[u])
            fetch(1, [pair.at[u, r[1] + k * r[2]] for k in range(2)] + [l1.at[u, 2 + k] for k in range(2)], ac)

        def fetch_d(u, m, r):
            wait_like(l2.at[u], r2.at[u])
            fetch(2, [pair.at[u, r[2]], l1.at[u, 1], l2.at[u, 1]], ad)

        def fetch_e(u, m, r):
            wait_like(l3.at[u], r3.at[u])
            fetch(3, [pair.at[u, 0], l1.at[u, 0], l2.at[u, 0], l3.at[u, 0]], ae)

        at(LAG_B, fetch_b)
        at(LAG_C, fetch_c)
        at(LAG_D, fetch_d)
        at(LAG_E, fetch_e)

        def free(stage, u, src, slot):
            @pl.when(u >= 2)
            def _():
                wait_like(src, send_sem.at[stage, slot])

        def stage_a(u, m, r):
            for c in w_copies(u):
                c.wait()
            slot = lax.rem(u, 2)
            free(0, u, sa.at[slot], slot)
            for k in range(4):
                v = part(u, 8 + 2 * k, 2).astype(BF)
                sa[slot, 2 * k] = v[:SHARD]
                sa[slot, 2 * k + 1] = v[SHARD:]
            send(0, sa.at[slot], pair.at[u], pair_sem.at[u], partner, slot)

        def stage_b(u, m, r):
            slot = lax.rem(u, 2)
            wait_like(ab, load_sem.at[0])
            free(1, u, sb.at[slot], slot)
            for i in range(2):
                for k in range(2):
                    v = part(u, r[0] + i * r[1] + k * r[2]) + ab[2 * i + k].astype(F32)
                    sb[slot, 2 * i + k] = v.astype(BF)
            send(1, sb.at[slot], l1.at[u], r1.at[u], across(me, m[0]), slot)

        def stage_c(u, m, r):
            slot = lax.rem(u, 2)
            wait_like(ac, load_sem.at[1])
            free(2, u, sc.at[slot], slot)
            for k in range(2):
                v = part(u, r[1] + k * r[2]) + ac[k].astype(F32) + ac[2 + k].astype(F32)
                sc[slot, k] = v.astype(BF)
            send(2, sc.at[slot], l2.at[u], r2.at[u], across(me, m[1]), slot)

        def stage_d(u, m, r):
            slot = lax.rem(u, 2)
            wait_like(ad, load_sem.at[2])
            free(3, u, sd.at[slot], slot)
            v = part(u, r[2]) + ad[0].astype(F32) + ad[1].astype(F32) + ad[2].astype(F32)
            sd[slot, 0] = v.astype(BF)
            send(3, sd.at[slot], l3.at[u], r3.at[u], across(me, m[2]), slot)

        def stage_e(u, m, r):
            slot = lax.rem(u, 2)
            wait_like(ae, load_sem.at[3])

            @pl.when(u >= 2)
            def _():
                wait_like(se.at[slot], out_sem.at[slot])

            v = part(u, 0) + ae[0].astype(F32) + ae[1].astype(F32) + ae[2].astype(F32) + ae[3].astype(F32)
            se[slot] = v.astype(BF)
            cols = pl.ds(pl.multiple_of(u * E, E), E)
            pltpu.make_async_copy(se.at[slot], dx.at[:, cols], out_sem.at[slot]).start()

        at(0, stage_a)
        at(LAG_B, stage_b)
        at(LAG_C, stage_c)
        at(LAG_D, stage_d)
        at(LAG_E, stage_e)

    loop(0, STEPS + LAG_E, step)
    for slot in range(2):
        for stage, ref in enumerate((sa, sb, sc, sd)):
            wait_like(ref.at[slot], send_sem.at[stage, slot])
        wait_like(se.at[slot], out_sem.at[slot])


def call(kernel, outs, scratch, flops, args):
    moved = sum(a.size * a.dtype.itemsize for a in (*args, *outs))
    return pl.pallas_call(
        kernel,
        out_shape=outs,
        in_specs=[ANY] * len(args),
        out_specs=[ANY] * len(outs),
        scratch_shapes=scratch,
        cost_estimate=pl.CostEstimate(flops=flops, bytes_accessed=moved, transcendentals=0),
        compiler_params=pltpu.CompilerParams(has_side_effects=True, vmem_limit_bytes=60 * 2**20),
    )(*args)


def solution(mesh):
    sds = jax.ShapeDtypeStruct
    dma = pltpu.SemaphoreType.DMA
    product = 2 * ROWS * D * F

    def step(x, dy, gate, up, w_gate, w_up, w_down):
        _, d, dw_down = call(
            hidden_kernel,
            [sds((N, SHARD, D), BF), sds((ROWS, 2 * F), BF), sds((F, D), BF)],
            [
                pltpu.VMEM((ROWS, F), F32),
                pltpu.VMEM((F, ROWS), BF),
                pltpu.VMEM((2, ROWS, C), BF),
                pltpu.VMEM((2, F, C), BF),
                pltpu.VMEM((2, F, C), BF),
                pltpu.VMEM((2, 2, T, F), BF),
                pltpu.VMEM((2, T, 2 * F), BF),
                *Gather.SEMS,
                dma((2,)),
                dma((2,)),
                dma((2,)),
                dma((2,)),
            ],
            2 * product,
            (dy, gate, up, w_down),
        )
        dx, *_ = call(
            sum_kernel,
            [sds((SHARD, D), BF)] + [sds((STEPS, n, SHARD, E), BF) for n in (8, 4, 2, 1)],
            [
                pltpu.VMEM((D, 2 * F), BF),
                pltpu.VMEM((ROWS, 2 * F), BF),
                *[pltpu.VMEM((2, n, SHARD, E), BF) for n in (8, 4, 2, 1)],
                pltpu.VMEM((2, SHARD, E), BF),
                *[pltpu.VMEM((n, SHARD, E), BF) for n in (4, 4, 3, 4)],
                dma,
                dma((2, STEPS)),
                dma((STEPS,)),
                dma((STEPS,)),
                dma((STEPS,)),
                dma((STEPS,)),
                dma((4, 2)),
                dma((4,)),
                dma((2,)),
            ],
            2 * product,
            (d, w_gate, w_up),
        )
        _, dw_gate, dw_up = call(
            weights_kernel,
            [sds((N, SHARD, D), BF), sds((D, F), BF), sds((D, F), BF)],
            [
                pltpu.VMEM((2, ROWS, C), BF),
                pltpu.VMEM((ROWS, 2 * F), BF),
                pltpu.VMEM((2, 2, C, F), BF),
                *Gather.SEMS,
                dma,
                dma((2,)),
            ],
            2 * product,
            (x, d),
        )
        return dx, dw_gate, dw_up, dw_down

    rows, cols = P(("dp", "tp"), None), P("dp", "tp")
    weight, down = P(None, "tp"), P("tp", None)
    return jax.shard_map(
        step,
        mesh=mesh,
        in_specs=(rows, rows, cols, cols, weight, weight, down),
        out_specs=(rows, cols, cols, rows),
        check_vma=False,
    )
```

```python
import jax
import jax.numpy as jnp
from jax import lax
from jax.experimental import pallas as pl
from jax.experimental.pallas import tpu as pltpu
from jax.sharding import PartitionSpec as P

ROWS, D, FF, N = 2560, 7168, 18432, 16
SHARD, F = ROWS // N, FF // N
CY, CX = 512, 256
CHUNKS = D // CY
PIECES = ((0, 56), (56, 56), (112, 48))
T = 256
TILES = ROWS // T
E = 256
STEPS = D // E
LAG_B, LAG_C, LAG_D, LAG_E = 1, 3, 5, 7
LAG_X = 3
LEADS_X = (10, 6, 2, 16)
X_FROM = 8
BF, F32 = jnp.bfloat16, jnp.float32
NT = (((1,), (1,)), ((), ()))
TN = (((0,), (0,)), ((), ()))
ANY = pl.BlockSpec(memory_space=pl.ANY)


def dot(a, b, dims=(((1,), (0,)), ((), ()))):
    return lax.dot_general(a, b, dims, preferred_element_type=F32)


def across(device, mask):
    return device + mask * (1 - 2 * lax.rem(lax.div(device, jnp.int32(mask)), jnp.int32(2)))


def axis_mask(i):
    return 8 - 5 * i + i * i


def masks(start):
    i = [lax.rem(jnp.int32(start + k), jnp.int32(3)) for k in range(3)]
    return [axis_mask(k) for k in i]


def loop(lo, hi, body):
    lax.fori_loop(lo, hi, lambda i, c: (body(i), c)[1], 0)


class Gather:
    @staticmethod
    def sems(c):
        n = D // c
        return [pltpu.SemaphoreType.DMA(s) for s in ((3, 3 * n), (n,), (n,), (2,))]

    def __init__(self, own, g, buf, c, leads, place, arrived, paired, sent, loaded):
        self.own_ref, self.g, self.buf, self.c, self.leads, self.place = own, g, buf, c, leads, place
        self.arrived, self.paired, self.sent, self.loaded = arrived, paired, sent, loaded
        self.me = lax.axis_index("tp").astype(jnp.int32)
        self.chunks = D // c

    def cols(self, j):
        return pl.ds(pl.multiple_of(j * self.c, self.c), self.c)

    def send(self, j, q, shard, to, phase, src=None):
        rows = pl.ds(*PIECES[q])
        place = self.g.at[shard, rows, self.cols(j)]
        src = place if src is None else src.at[rows, self.cols(j)]
        sem = self.paired.at[j] if phase == 3 else self.arrived.at[phase, 3 * j + q]
        pltpu.make_async_remote_copy(
            src, place, self.sent.at[j], sem, device_id={"tp": to}, device_id_type=pl.DeviceIdType.MESH
        ).start()

    def wait(self, sem, shards, rows):
        ref = self.g.at[pl.ds(0, shards), pl.ds(0, rows), pl.ds(0, self.c)]
        pltpu.make_async_copy(ref, ref, sem).wait()

    def first(self, j):
        for q in range(3):
            m = masks(j + q)
            for phase in range(3):
                self.send(j, q, self.me, across(self.me, m[phase]), phase, self.own_ref)
            self.send(j, q, self.me, across(self.me, 1), 3, self.own_ref)

    def forward(self, phase, j):
        for q in range(3):
            self.wait(self.arrived.at[phase, 3 * j + q], 2**phase, PIECES[q][1])
            m = masks(j + q)
            shards = [across(self.me, m[phase])]
            for earlier in range(phase):
                shards += [across(s, m[earlier]) for s in shards]
            for s in shards:
                for later in range(phase + 1, 3):
                    self.send(j, q, s, across(self.me, m[later]), later)
                self.send(j, q, s, across(self.me, 1), 3)

    def load(self, j):
        self.wait(self.paired.at[j], 8, SHARD)
        slot = lax.rem(j, 2)
        for r in range(N):
            device, at = self.place(r)
            src = self.own_ref.at[:, self.cols(j)] if r == 0 else self.g.at[device, :, self.cols(j)]
            dst = self.buf.at[slot, pl.ds(pl.multiple_of(at * SHARD, SHARD), SHARD)]
            pltpu.make_async_copy(src, dst, self.loaded.at[slot]).start()

    def guarded(self, j, f):
        @pl.when((j >= 0) & (j < self.chunks))
        def _():
            f(j)

    def pump(self, t):
        for phase in (2, 1, 0):
            self.guarded(t + self.leads[phase], lambda j: self.forward(phase, j))
        self.guarded(t + self.leads[3], self.first)

    def held(self, j):
        slot = lax.rem(j, 2)
        ref = self.buf.at[slot]
        pltpu.make_async_copy(ref, ref, self.loaded.at[slot]).wait()
        return slot

    def finish(self):
        loop(0, self.chunks, lambda j: self.wait(self.sent.at[j], 15, SHARD))


def wait_like(ref, sem):
    pltpu.make_async_copy(ref, ref, sem).wait()


def relative(me, p):
    device = across(me, 1) if p >= 8 else me
    for bit in (1, 2, 4):
        if p & bit:
            device = across(device, 2 * bit)
    return device


def kernel(*refs):
    it = iter(refs)
    take = lambda n: [next(it) for _ in range(n)]
    x, dy, gate, up, w_gate, w_up, w_down = take(7)
    dx, dwg, dwu, dwd, gy, gx, pair, l1, l2, l3 = take(10)
    d, acc, ht, ybuf, wd, o, kept = take(7)
    w, xbuf, sa, sb, sc, sd, se, ab, ac, ad, ae = take(11)
    y_sems, x_sems = take(4), take(4)
    wd_sem, o_sem, kept_sem, ox_sem = take(4)
    w_sem, pair_sem, r1, r2, r3, send_sem, load_sem, out_sem = take(8)
    me = lax.axis_index("tp").astype(jnp.int32)
    partner = across(me, 1)

    def absolute(r):
        s = lax.rem(me + r, jnp.int32(N))
        return s, s

    y = Gather(dy, gy, ybuf, CY, (4, 3, 2, 7), absolute, *y_sems)
    xg = Gather(x, gx, xbuf, CX, LEADS_X, lambda p: (relative(me, p), p), *x_sems)

    for j in range(3):
        y.first(jnp.int32(j))

    def fetch(slot, start, rows):
        span = pl.ds(start, rows)
        for k, ref in enumerate((gate, up)):
            pltpu.make_async_copy(ref.at[span], kept.at[slot, k, pl.ds(0, rows)], kept_sem.at[slot]).start()

    def fetched(slot, rows):
        wait_like(kept.at[slot, :, pl.ds(0, rows)], kept_sem.at[slot])
        return [kept[slot, k, :rows].astype(F32) for k in range(2)]

    def wd_fetch(j):
        slot = lax.rem(j, 2)
        pltpu.make_async_copy(w_down.at[:, y.cols(j)], wd.at[slot], wd_sem.at[slot]).start()

    fetch(0, 0, T)
    wd_fetch(jnp.int32(0))

    def hide(i):
        slot, rows = lax.rem(i, 2), pl.ds(pl.multiple_of(i * T, T), T)

        @pl.when(i + 1 < TILES)
        def _():
            fetch(1 - slot, pl.multiple_of((i + 1) * T, T), T)

        gt, ut = fetched(slot, T)
        ht[:, rows] = (gt * jax.nn.sigmoid(gt) * ut).T.astype(BF)
        acc[rows, :] = jnp.zeros((T, F), F32)

        @pl.when((lax.rem(i, 2) == 1) & (i < 8))
        def _():
            t = lax.div(i, 2) - 4
            y.guarded(t + 1, y.load)
            y.pump(t)

    loop(0, TILES, hide)

    def chunk(j):
        y.guarded(j + 1, y.load)
        y.pump(j)

        @pl.when(j >= X_FROM)
        def _():
            for k in range(2):
                xg.pump(2 * (j - X_FROM) - LEADS_X[3] + k)

        @pl.when(j + 1 < CHUNKS)
        def _():
            wd_fetch(j + 1)

        slot = y.held(j)
        wait_like(wd.at[slot], wd_sem.at[slot])

        def rows_of(i):
            rows = pl.ds(pl.multiple_of(i * (ROWS // 2), ROWS // 2), ROWS // 2)
            acc[rows, :] += dot(ybuf[slot, rows, :], wd[slot], NT)

        loop(0, 2, rows_of)

        @pl.when(j >= 2)
        def _():
            wait_like(o.at[slot], o_sem.at[slot])

        o[slot] = dot(ht[...], ybuf[slot]).astype(BF)
        pltpu.make_async_copy(o.at[slot], dwd.at[:, y.cols(j)], o_sem.at[slot]).start()

    loop(0, CHUNKS, chunk)

    sent_x = 2 * (CHUNKS - X_FROM) - LEADS_X[3]
    fetch(0, pl.multiple_of(me * SHARD, SHARD), SHARD)
    for p in range(N):
        slot, start = p % 2, pl.multiple_of(relative(me, p) * SHARD, SHARD)
        if p + 1 < N:
            fetch(1 - slot, pl.multiple_of(relative(me, p + 1) * SHARD, SHARD), SHARD)
        gt, ut = fetched(slot, SHARD)
        dh, s = acc[pl.ds(start, SHARD), :], jax.nn.sigmoid(gt)
        rows = pl.ds(p * SHARD, SHARD)
        d[rows, :F] = (dh * ut * (s * (1 + gt * (1 - s)))).astype(BF)
        d[rows, F:] = (dh * (gt * s)).astype(BF)
        if p % 3 == 2:
            xg.pump(jnp.int32(sent_x + p // 3))
    pumped = sent_x + N // 3

    def w_start(t):
        rows, slot = pl.ds(pl.multiple_of(t * E, E), E), lax.rem(t, 3)
        for k, ref in enumerate((w_gate, w_up)):
            pltpu.make_async_copy(ref.at[rows], w.at[slot, :, pl.ds(k * F, F)], w_sem.at[slot]).start()

    def part(t, half):
        return dot(d[pl.ds(half * (ROWS // 2), ROWS // 2), :], w[lax.rem(t, 3)], NT)

    def held(u, block):
        slot = lax.rem(u, 8)
        row = lax.rem(slot, 2) * (ROWS // 2) + block * SHARD
        col = pl.multiple_of(lax.div(slot, 2) * E, E)
        return pl.ds(pl.multiple_of(row, SHARD), SHARD), pl.ds(col, E)

    def send(stage, src, dst, recv, to, slot):
        pltpu.make_async_remote_copy(
            src, dst, send_sem.at[stage, slot], recv, device_id={"tp": to}, device_id_type=pl.DeviceIdType.MESH
        ).start()

    def free(stage, u, src, slot):
        @pl.when(u >= 2)
        def _():
            wait_like(src, send_sem.at[stage, slot])

    def step(t):
        def at(lag, f):
            u = t - lag

            @pl.when((u >= 0) & (u < STEPS))
            def _():
                m = masks(u)
                f(u, m, [lax.div(k, 2) for k in m])

        def get(stage, srcs, buf):
            for k, s in enumerate(srcs):
                pltpu.make_async_copy(s, buf.at[k], load_sem.at[stage]).start()

        def get_b(u, m, r):
            wait_like(pair.at[u], pair_sem.at[u])
            pltpu.make_async_copy(pair.at[u], ab, load_sem.at[0]).start()

        def get_c(u, m, r):
            wait_like(l1.at[u], r1.at[u])
            get(1, [l1.at[u, 2 + k] for k in range(2)], ac)

        def get_d(u, m, r):
            wait_like(l2.at[u], r2.at[u])
            get(2, [l1.at[u, 1], l2.at[u, 1]], ad)

        def get_e(u, m, r):
            wait_like(l3.at[u], r3.at[u])
            get(3, [l1.at[u, 0], l2.at[u, 0], l3.at[u, 0]], ae)

        def stage_a(u, m, r):
            wait_like(w.at[lax.rem(u, 3)], w_sem.at[lax.rem(u, 3)])
            slot = lax.rem(u, 2)
            free(0, u, sa.at[slot], slot)
            sa[slot] = part(u, 1).astype(BF)
            send(0, sa.at[slot], pair.at[u], pair_sem.at[u], partner, slot)

        def stage_b(u, m, r):
            slot = lax.rem(u, 2)
            wait_like(ab, load_sem.at[0])
            free(1, u, sb.at[slot], slot)
            row, col = held(u, 0)
            acc[pl.ds(row.start, ROWS // 2), col] = part(u, 0) + ab[...].astype(F32)
            for i in range(2):
                for k in range(2):
                    sb[slot, 2 * i + k] = acc[held(u, r[0] + i * r[1] + k * r[2])].astype(BF)
            send(1, sb.at[slot], l1.at[u], r1.at[u], across(me, m[0]), slot)

        def stage_c(u, m, r):
            slot = lax.rem(u, 2)
            wait_like(ac, load_sem.at[1])
            free(2, u, sc.at[slot], slot)
            for k in range(2):
                sc[slot, k] = (acc[held(u, r[1] + k * r[2])] + ac[k].astype(F32)).astype(BF)
            send(2, sc.at[slot], l2.at[u], r2.at[u], across(me, m[1]), slot)

        def stage_d(u, m, r):
            slot = lax.rem(u, 2)
            wait_like(ad, load_sem.at[2])
            free(3, u, sd.at[slot], slot)
            sd[slot, 0] = (acc[held(u, r[2])] + ad[0].astype(F32) + ad[1].astype(F32)).astype(BF)
            send(3, sd.at[slot], l3.at[u], r3.at[u], across(me, m[2]), slot)

        def stage_e(u, m, r):
            slot = lax.rem(u, 2)
            wait_like(ae, load_sem.at[3])

            @pl.when(u >= 2)
            def _():
                wait_like(se.at[slot], out_sem.at[slot])

            v = acc[held(u, 0)] + ae[0].astype(F32) + ae[1].astype(F32) + ae[2].astype(F32)
            se[slot] = v.astype(BF)
            pltpu.make_async_copy(se.at[slot], dx.at[:, pl.ds(pl.multiple_of(u * E, E), E)], out_sem.at[slot]).start()

        def weights(u, m, r):
            slot = xg.held(u)

            @pl.when(u >= 2)
            def _():
                wait_like(kept.at[slot], ox_sem.at[slot])

            v = dot(xbuf[slot], d[...], TN)
            rows = pl.ds(pl.multiple_of(u * CX, CX), CX)
            for k, ref in enumerate((dwg, dwu)):
                kept[slot, k] = v[:, k * F : (k + 1) * F].astype(BF)
                pltpu.make_async_copy(kept.at[slot, k], ref.at[rows], ox_sem.at[slot]).start()

        @pl.when(t + 1 < STEPS)
        def _():
            w_start(t + 1)

        at(LAG_X - 1, lambda u, m, r: xg.load(u))
        at(LAG_B, get_b)
        at(LAG_C, get_c)
        at(LAG_D, get_d)
        at(LAG_E, get_e)
        at(0, stage_a)
        at(LAG_B, stage_b)
        at(LAG_C, stage_c)
        at(LAG_D, stage_d)
        at(LAG_E, stage_e)
        xg.pump(t + pumped)
        at(LAG_X, weights)

    w_start(jnp.int32(0))
    loop(0, STEPS + max(LAG_E, LAG_X), step)
    for slot in range(2):
        for stage, ref in enumerate((sa, sb, sc, sd)):
            wait_like(ref.at[slot], send_sem.at[stage, slot])
        wait_like(se.at[slot], out_sem.at[slot])
        wait_like(o.at[slot], o_sem.at[slot])
        wait_like(kept.at[slot], ox_sem.at[slot])
    y.finish()
    xg.finish()


def solution(mesh):
    sds, vmem = jax.ShapeDtypeStruct, lambda *s: pltpu.VMEM(s, BF)
    dma = pltpu.SemaphoreType.DMA

    def step(*args):
        outs = [sds((SHARD, D), BF), sds((D, F), BF), sds((D, F), BF), sds((F, D), BF)]
        outs += [sds((N, SHARD, D), BF)] * 2
        outs += [sds((STEPS, ROWS // 2, E), BF)] + [sds((STEPS, n, SHARD, E), BF) for n in (4, 2, 1)]
        return pl.pallas_call(
            kernel,
            out_shape=outs,
            in_specs=[ANY] * len(args),
            out_specs=[ANY] * len(outs),
            scratch_shapes=[
                vmem(ROWS, 2 * F),
                pltpu.VMEM((ROWS, F), F32),
                vmem(F, ROWS),
                vmem(2, ROWS, CY),
                vmem(2, F, CY),
                vmem(2, F, CY),
                vmem(2, 2, T, F),
                vmem(3, E, 2 * F),
                vmem(2, ROWS, CX),
                vmem(2, ROWS // 2, E),
                *[vmem(2, n, SHARD, E) for n in (4, 2, 1)],
                vmem(2, SHARD, E),
                vmem(ROWS // 2, E),
                *[vmem(n, SHARD, E) for n in (2, 2, 3)],
                *Gather.sems(CY),
                *Gather.sems(CX),
                *[dma((2,))] * 4,
                dma((3,)),
                *[dma((STEPS,))] * 4,
                dma((4, 2)),
                dma((4,)),
                dma((2,)),
            ],
            cost_estimate=pl.CostEstimate(flops=12 * ROWS * D * F, bytes_accessed=400 * 2**20, transcendentals=0),
            compiler_params=pltpu.CompilerParams(has_side_effects=True, vmem_limit_bytes=63 * 2**20),
        )(*args)[:4]

    rows, cols = P(("dp", "tp"), None), P("dp", "tp")
    weight, down = P(None, "tp"), P("tp", None)
    return jax.shard_map(
        step,
        mesh=mesh,
        in_specs=(rows, rows, cols, cols, weight, weight, down),
        out_specs=(rows, cols, cols, rows),
        check_vma=False,
    )
```

```python
import jax
import jax.numpy as jnp
from jax import lax
from jax.experimental import pallas as pl
from jax.experimental.pallas import tpu as pltpu
from jax.sharding import PartitionSpec as P

ROWS, D, FF, N = 2560, 7168, 18432, 16
SHARD, F = ROWS // N, FF // N
C = 256
CW = 512
CHUNKS = D // CW
T = 256
TILES = ROWS // T
E = 256
STEPS = D // E
LAG_B, LAG_C, LAG_D, LAG_E = 1, 3, 5, 7
LAG_X = 1
LATE = 8
EARLY = D // C - LATE
HELD = 6
LEADS_Y = (8, 6, 4, 12)
LEADS_X = (11, 6, 2, 16)
X_FROM = 8
BF, F32 = jnp.bfloat16, jnp.float32
NT = (((1,), (1,)), ((), ()))
TN = (((0,), (0,)), ((), ()))
ANY = pl.BlockSpec(memory_space=pl.ANY)


def dot(a, b, dims=(((1,), (0,)), ((), ()))):
    return lax.dot_general(a, b, dims, preferred_element_type=F32)


def across(device, mask):
    return device + mask * (1 - 2 * lax.rem(lax.div(device, jnp.int32(mask)), jnp.int32(2)))


def axis_mask(i):
    return 8 - 5 * i + i * i


def masks(start):
    i = [lax.rem(jnp.int32(start + k), jnp.int32(3)) for k in range(3)]
    return [axis_mask(k) for k in i]


def loop(lo, hi, body):
    lax.fori_loop(lo, hi, lambda i, c: (body(i), c)[1], 0)


class Gather:
    CHUNKS = D // C
    SEMS = [pltpu.SemaphoreType.DMA(s) for s in ((3, CHUNKS), (CHUNKS,), (CHUNKS,), (2,))]

    def __init__(self, own, g, buf, leads, relative, arrived, paired, sent, loaded):
        self.own_ref, self.g, self.buf, self.leads, self.relative = own, g, buf, leads, relative
        self.arrived, self.paired, self.sent, self.loaded = arrived, paired, sent, loaded
        self.me = lax.axis_index("tp").astype(jnp.int32)
        self.width = buf.shape[-1] // C

    def send(self, j, src, half, r, to, sem):
        pltpu.make_async_remote_copy(
            src, self.g.at[half, j, r], self.sent.at[j], sem, device_id={"tp": to}, device_id_type=pl.DeviceIdType.MESH
        ).start()

    def wait(self, sem, shards):
        ref = self.own_ref.at[:, pl.ds(0, shards * C)]
        pltpu.make_async_copy(ref, ref, sem).wait()

    def own(self, j):
        return self.own_ref.at[:, pl.ds(pl.multiple_of(j * C, C), C)]

    def first(self, j):
        m = masks(j)
        for phase in range(3):
            self.send(j, self.own(j), 0, 2**phase, across(self.me, m[phase]), self.arrived.at[phase, j])
        self.send(j, self.own(j), 1, 0, across(self.me, 1), self.paired.at[j])

    def forward(self, phase, j):
        self.wait(self.arrived.at[phase, j], 2**phase)
        m = masks(j)
        if phase == 0:
            for later in (1, 2):
                self.send(j, self.g.at[0, j, 1], 0, 1 + 2**later, across(self.me, m[later]), self.arrived.at[later, j])
        elif phase == 1:
            self.send(j, self.g.at[0, j, pl.ds(2, 2)], 0, pl.ds(6, 2), across(self.me, m[2]), self.arrived.at[2, j])
        else:
            self.send(j, self.g.at[0, j, pl.ds(1, 7)], 1, pl.ds(1, 7), across(self.me, 1), self.paired.at[j])

    def copies(self, j, dst, sem):
        m = masks(j)
        out = []
        for half in range(2):
            for r in range(8):
                device, block = across(self.me, 1) if half else self.me, jnp.int32(8 * half)
                for k in range(3):
                    if r & (1 << k):
                        device, block = across(device, m[k]), block + lax.div(m[k], jnp.int32(2))
                at = pl.multiple_of((block if self.relative else device) * SHARD, SHARD)
                src = self.g.at[half, j, r] if half or r else self.own(j)
                out.append(pltpu.make_async_copy(src, dst(pl.ds(at, SHARD)), sem))
        return out

    def load(self, j):
        self.wait(self.paired.at[j], 8)
        slot = lax.rem(lax.div(j, jnp.int32(self.width)), 2)
        cols = pl.ds(pl.multiple_of(lax.rem(j, jnp.int32(self.width)) * C, C), C)
        for c in self.copies(j, lambda rows: self.buf.at[slot, rows, cols], self.loaded.at[slot]):
            c.start()

    def guarded(self, j, f):
        @pl.when((j >= 0) & (j < self.CHUNKS))
        def _():
            f(j)

    def pump(self, t):
        for phase in (2, 1, 0):
            self.guarded(t + self.leads[phase], lambda j: self.forward(phase, j))
        self.guarded(t + self.leads[3], self.first)

    def held(self, j):
        slot = lax.rem(j, 2)
        ref = self.buf.at[slot]
        pltpu.make_async_copy(ref, ref, self.loaded.at[slot]).wait()
        return slot

    def finish(self):
        loop(0, self.CHUNKS, lambda j: self.wait(self.sent.at[j], 15))


def wait_like(ref, sem):
    pltpu.make_async_copy(ref, ref, sem).wait()


def relative(me, p):
    device = across(me, 1) if p >= 8 else me
    for bit in (1, 2, 4):
        if p & bit:
            device = across(device, 2 * bit)
    return device


def main_kernel(*refs):
    it = iter(refs)
    take = lambda n: [next(it) for _ in range(n)]
    x, dy, gate, up, w_gate, w_up, w_down = take(7)
    dx, dwg, dwu, dwd, d_out, gy, gx, pair, l1, l2, l3 = take(11)
    d, acc, ht, ybuf, wd, o, kept = take(7)
    w, xbuf, sa, sb, sc, sd, se, ab, ac, ad, ae = take(11)
    y_sems, x_sems = take(4), take(4)
    wd_sem, o_sem, kept_sem, ox_sem, d_sem = take(5)
    w_sem, pair_sem, r1, r2, r3, send_sem, load_sem, out_sem = take(8)
    me = lax.axis_index("tp").astype(jnp.int32)
    partner = across(me, 1)

    y = Gather(dy, gy, ybuf, LEADS_Y, False, *y_sems)
    xg = Gather(x, gx, xbuf, LEADS_X, True, *x_sems)

    for j in range(LEADS_Y[3] - TILES):
        y.first(jnp.int32(j))

    def fetch(slot, start, rows):
        span = pl.ds(start, rows)
        for k, ref in enumerate((gate, up)):
            pltpu.make_async_copy(ref.at[span], kept.at[slot, k, pl.ds(0, rows)], kept_sem.at[slot]).start()

    def fetched(slot, rows):
        wait_like(kept.at[slot, :, pl.ds(0, rows)], kept_sem.at[slot])
        return [kept[slot, k, :rows].astype(F32) for k in range(2)]

    def wide(j):
        return pl.ds(pl.multiple_of(j * CW, CW), CW)

    def wd_fetch(j):
        slot = lax.rem(j, 2)
        pltpu.make_async_copy(w_down.at[:, wide(j)], wd.at[slot], wd_sem.at[slot]).start()

    fetch(0, 0, T)
    wd_fetch(jnp.int32(0))

    def pump_y(t):
        y.guarded(t + 2, y.load)
        y.pump(t)

    def hide(i):
        slot, rows = lax.rem(i, 2), pl.ds(pl.multiple_of(i * T, T), T)

        @pl.when(i + 1 < TILES)
        def _():
            fetch(1 - slot, pl.multiple_of((i + 1) * T, T), T)

        gt, ut = fetched(slot, T)
        ht[:, rows] = (gt * jax.nn.sigmoid(gt) * ut).T.astype(BF)
        acc[rows, :] = jnp.zeros((T, F), F32)

        pump_y(i - TILES)

    loop(0, TILES, hide)

    def chunk(j):
        pump_y(2 * j)

        @pl.when(j >= X_FROM)
        def _():
            for k in range(2):
                xg.pump(2 * (j - X_FROM) - LEADS_X[3] + k)

        @pl.when(j + 1 < CHUNKS)
        def _():
            wd_fetch(j + 1)

        slot = y.held(j)
        wait_like(wd.at[slot], wd_sem.at[slot])

        def rows_of(i):
            rows = pl.ds(pl.multiple_of(i * (ROWS // 2), ROWS // 2), ROWS // 2)
            acc[rows, :] += dot(ybuf[slot, rows, :], wd[slot], NT)

        loop(0, 2, rows_of)
        pump_y(2 * j + 1)

        @pl.when(j >= 2)
        def _():
            wait_like(o.at[slot], o_sem.at[slot])

        o[slot] = dot(ht[...], ybuf[slot]).astype(BF)
        pltpu.make_async_copy(o.at[slot], dwd.at[:, wide(j)], o_sem.at[slot]).start()

    loop(0, CHUNKS, chunk)

    sent_x = 2 * (CHUNKS - X_FROM) - LEADS_X[3]
    fetch(0, pl.multiple_of(me * SHARD, SHARD), SHARD)
    for p in range(N):
        slot, start = p % 2, pl.multiple_of(relative(me, p) * SHARD, SHARD)
        if p + 1 < N:
            fetch(1 - slot, pl.multiple_of(relative(me, p + 1) * SHARD, SHARD), SHARD)
        gt, ut = fetched(slot, SHARD)
        dh, s = acc[pl.ds(start, SHARD), :], jax.nn.sigmoid(gt)
        rows = pl.ds(p * SHARD, SHARD)
        d[rows, :F] = (dh * ut * (s * (1 + gt * (1 - s)))).astype(BF)
        d[rows, F:] = (dh * (gt * s)).astype(BF)
        if p % 3 == 2:
            xg.pump(jnp.int32(sent_x + p // 3))
    pumped = sent_x + N // 3
    pltpu.make_async_copy(d, d_out, d_sem).start()

    def w_start(t):
        rows, slot = pl.ds(pl.multiple_of(t * E, E), E), lax.rem(t, 3)
        for k, ref in enumerate((w_gate, w_up)):
            pltpu.make_async_copy(ref.at[rows], w.at[slot, :, pl.ds(k * F, F)], w_sem.at[slot]).start()

    def part(t, half):
        return dot(d[pl.ds(half * (ROWS // 2), ROWS // 2), :], w[lax.rem(t, 3)], NT)

    def held(u, block):
        slot = lax.rem(u, 8)
        row = lax.rem(slot, 2) * (ROWS // 2) + block * SHARD
        col = pl.multiple_of(lax.div(slot, 2) * E, E)
        return pl.ds(pl.multiple_of(row, SHARD), SHARD), pl.ds(col, E)

    def send(stage, src, dst, recv, to, slot):
        pltpu.make_async_remote_copy(
            src, dst, send_sem.at[stage, slot], recv, device_id={"tp": to}, device_id_type=pl.DeviceIdType.MESH
        ).start()

    def free(stage, u, src, slot):
        @pl.when(u >= 2)
        def _():
            wait_like(src, send_sem.at[stage, slot])

    def step(t):
        def at(lag, f):
            u = t - lag

            @pl.when((u >= 0) & (u < STEPS))
            def _():
                m = masks(u)
                f(u, m, [lax.div(k, 2) for k in m])

        def get(stage, srcs, buf):
            for k, s in enumerate(srcs):
                pltpu.make_async_copy(s, buf.at[k], load_sem.at[stage]).start()

        def get_b(u, m, r):
            wait_like(pair.at[u], pair_sem.at[u])
            pltpu.make_async_copy(pair.at[u], ab, load_sem.at[0]).start()

        def get_c(u, m, r):
            wait_like(l1.at[u], r1.at[u])
            get(1, [l1.at[u, 2 + k] for k in range(2)], ac)

        def get_d(u, m, r):
            wait_like(l2.at[u], r2.at[u])
            get(2, [l1.at[u, 1], l2.at[u, 1]], ad)

        def get_e(u, m, r):
            wait_like(l3.at[u], r3.at[u])
            get(3, [l1.at[u, 0], l2.at[u, 0], l3.at[u, 0]], ae)

        def stage_a(u, m, r):
            wait_like(w.at[lax.rem(u, 3)], w_sem.at[lax.rem(u, 3)])
            slot = lax.rem(u, 2)
            free(0, u, sa.at[slot], slot)
            sa[slot] = part(u, 1).astype(BF)
            send(0, sa.at[slot], pair.at[u], pair_sem.at[u], partner, slot)

        def stage_b(u, m, r):
            slot = lax.rem(u, 2)
            wait_like(ab, load_sem.at[0])
            free(1, u, sb.at[slot], slot)
            row, col = held(u, 0)
            acc[pl.ds(row.start, ROWS // 2), col] = part(u, 0) + ab[...].astype(F32)
            for i in range(2):
                for k in range(2):
                    sb[slot, 2 * i + k] = acc[held(u, r[0] + i * r[1] + k * r[2])].astype(BF)
            send(1, sb.at[slot], l1.at[u], r1.at[u], across(me, m[0]), slot)

        def stage_c(u, m, r):
            slot = lax.rem(u, 2)
            wait_like(ac, load_sem.at[1])
            free(2, u, sc.at[slot], slot)
            for k in range(2):
                sc[slot, k] = (acc[held(u, r[1] + k * r[2])] + ac[k].astype(F32)).astype(BF)
            send(2, sc.at[slot], l2.at[u], r2.at[u], across(me, m[1]), slot)

        def stage_d(u, m, r):
            slot = lax.rem(u, 2)
            wait_like(ad, load_sem.at[2])
            free(3, u, sd.at[slot], slot)
            sd[slot, 0] = (acc[held(u, r[2])] + ad[0].astype(F32) + ad[1].astype(F32)).astype(BF)
            send(3, sd.at[slot], l3.at[u], r3.at[u], across(me, m[2]), slot)

        def stage_e(u, m, r):
            slot = lax.rem(u, 2)
            wait_like(ae, load_sem.at[3])

            @pl.when(u >= 2)
            def _():
                wait_like(se.at[slot], out_sem.at[slot])

            v = acc[held(u, 0)] + ae[0].astype(F32) + ae[1].astype(F32) + ae[2].astype(F32)
            se[slot] = v.astype(BF)
            pltpu.make_async_copy(se.at[slot], dx.at[:, pl.ds(pl.multiple_of(u * E, E), E)], out_sem.at[slot]).start()

        def due(t, f):
            last = lax.div(t, jnp.int32(STEPS))
            u = t - LAG_X + last * (EARLY - HELD - STEPS + LAG_X)

            @pl.when((u >= 0) & (u < EARLY - HELD * (1 - last)))
            def _():
                f(u)

        def weights(u):
            slot = xg.held(u)

            @pl.when(u >= 2)
            def _():
                wait_like(kept.at[slot], ox_sem.at[slot])

            v = dot(xbuf[slot], d[...], TN)
            rows = pl.ds(pl.multiple_of(u * C, C), C)
            for k, ref in enumerate((dwg, dwu)):
                kept[slot, k] = v[:, k * F : (k + 1) * F].astype(BF)
                pltpu.make_async_copy(kept.at[slot, k], ref.at[rows], ox_sem.at[slot]).start()

        @pl.when(t + 1 < STEPS)
        def _():
            w_start(t + 1)

        due(t + 1, xg.load)
        at(LAG_B, get_b)
        at(LAG_C, get_c)
        at(LAG_D, get_d)
        at(LAG_E, get_e)
        at(0, stage_a)
        at(LAG_B, stage_b)
        at(LAG_C, stage_c)
        at(LAG_D, stage_d)
        at(LAG_E, stage_e)
        xg.pump(t + pumped)
        due(t, weights)

    w_start(jnp.int32(0))
    loop(0, STEPS + LAG_E, step)
    for slot in range(2):
        for stage, ref in enumerate((sa, sb, sc, sd)):
            wait_like(ref.at[slot], send_sem.at[stage, slot])
        wait_like(se.at[slot], out_sem.at[slot])
        wait_like(o.at[slot], o_sem.at[slot])
        wait_like(kept.at[slot], ox_sem.at[slot])
    loop(EARLY, xg.CHUNKS, lambda j: xg.wait(xg.paired.at[j], 8))
    wait_like(d, d_sem)
    y.finish()
    xg.finish()


def last_kernel(*refs):
    it = iter(refs)
    take = lambda n: [next(it) for _ in range(n)]
    x, gx, d_in, dx_in, *finished = take(7)
    dx, *outs = take(4)
    d, xbuf, o, dxbuf, *bufs = take(7)
    d_sem, x_sem, o_sem, dx_sem, in_sem, out_sem = take(6)

    xg = Gather(x, gx, xbuf, None, True, None, None, None, None)

    def load(u):
        slot = lax.rem(u, 2)
        for c in xg.copies(EARLY + u, lambda rows: xbuf.at[slot, rows], x_sem.at[slot]):
            c.start()

    def piece(buf, u):
        rows = buf.shape[1]
        return pl.ds(pl.multiple_of(u * rows, rows), rows)

    def bring(u):
        for k in range(3):
            slot = lax.rem(u, 3)
            src = finished[k].at[piece(bufs[k], u)]
            pltpu.make_async_copy(src, bufs[k].at[slot], in_sem.at[k, slot]).start()

    pltpu.make_async_copy(d_in, d, d_sem).start()
    load(jnp.int32(0))
    pltpu.make_async_copy(dx_in, dxbuf, dx_sem).start()
    bring(jnp.int32(0))
    bring(jnp.int32(1))
    wait_like(d, d_sem)

    def step(u):
        slot, ring = lax.rem(u, 2), lax.rem(u, 3)

        @pl.when(u + 1 < LATE)
        def _():
            load(u + 1)

        for k in range(3):
            wait_like(bufs[k].at[ring], in_sem.at[k, ring])
            pltpu.make_async_copy(bufs[k].at[ring], outs[k].at[piece(bufs[k], u)], out_sem.at[k, ring]).start()

        @pl.when(u >= 1)
        def _():
            before = lax.rem(u + 2, 3)
            for k in range(3):
                wait_like(bufs[k].at[before], out_sem.at[k, before])

        @pl.when(u + 2 < LATE)
        def _():
            bring(u + 2)

        @pl.when(u == 1)
        def _():
            wait_like(dxbuf, dx_sem)
            pltpu.make_async_copy(dxbuf, dx, dx_sem).start()

        wait_like(xbuf.at[slot], x_sem.at[slot])

        @pl.when(u >= 2)
        def _():
            wait_like(o.at[slot], o_sem.at[slot])

        v = dot(xbuf[slot], d[...], TN)
        rows = pl.ds(pl.multiple_of((EARLY + u) * C, C), C)
        for k in range(2):
            o[slot, k] = v[:, k * F : (k + 1) * F].astype(BF)
            pltpu.make_async_copy(o.at[slot, k], outs[k].at[rows], o_sem.at[slot]).start()

    loop(0, LATE, step)
    for k in range(3):
        wait_like(bufs[k].at[(LATE - 1) % 3], out_sem.at[k, (LATE - 1) % 3])
    for slot in range(2):
        wait_like(o.at[slot], o_sem.at[slot])
    wait_like(dxbuf, dx_sem)


def solution(mesh):
    sds, vmem = jax.ShapeDtypeStruct, lambda *s: pltpu.VMEM(s, BF)
    dma = pltpu.SemaphoreType.DMA

    def call(kernel, outs, scratch, products, args, **params):
        return pl.pallas_call(
            kernel,
            out_shape=outs,
            in_specs=[ANY] * len(args),
            out_specs=[ANY] * len(outs),
            scratch_shapes=scratch,
            cost_estimate=pl.CostEstimate(flops=products * ROWS * D * F, bytes_accessed=2**28, transcendentals=0),
            compiler_params=pltpu.CompilerParams(vmem_limit_bytes=63 * 2**20, **params),
        )(*args)

    def step(x, dy, gate, up, w_gate, w_up, w_down):
        early = EARLY * C
        dx, dwg, dwu, dwd, d, _, gx, *_ = call(
            main_kernel,
            [sds((SHARD, D), BF), sds((early, F), BF), sds((early, F), BF), sds((F, D), BF), sds((ROWS, 2 * F), BF)]
            + [sds((2, D // C, 8, SHARD, C), BF)] * 2
            + [sds((STEPS, ROWS // 2, E), BF)]
            + [sds((STEPS, n, SHARD, E), BF) for n in (4, 2, 1)],
            [
                vmem(ROWS, 2 * F),
                pltpu.VMEM((ROWS, F), F32),
                vmem(F, ROWS),
                vmem(2, ROWS, CW),
                vmem(2, F, CW),
                vmem(2, F, CW),
                vmem(2, 2, T, F),
                vmem(3, E, 2 * F),
                vmem(2, ROWS, C),
                vmem(2, ROWS // 2, E),
                *[vmem(2, n, SHARD, E) for n in (4, 2, 1)],
                vmem(2, SHARD, E),
                vmem(ROWS // 2, E),
                *[vmem(n, SHARD, E) for n in (2, 2, 3)],
                *Gather.SEMS,
                *Gather.SEMS,
                *[dma((2,))] * 4,
                dma,
                dma((3,)),
                *[dma((STEPS,))] * 4,
                dma((4, 2)),
                dma((4,)),
                dma((2,)),
            ],
            11,
            (x, dy, gate, up, w_gate, w_up, w_down),
            has_side_effects=True,
        )
        dx, dwg, dwu, dwd = call(
            last_kernel,
            [sds((SHARD, D), BF), sds((D, F), BF), sds((D, F), BF), sds((F, D), BF)],
            [
                vmem(ROWS, 2 * F),
                vmem(2, ROWS, C),
                vmem(2, 2, C, F),
                vmem(SHARD, D),
                vmem(3, early // LATE, F),
                vmem(3, early // LATE, F),
                vmem(3, F // LATE, D),
                dma,
                dma((2,)),
                dma((2,)),
                dma,
                dma((3, 3)),
                dma((3, 3)),
            ],
            1,
            (x, gx, d, dx, dwg, dwu, dwd),
        )
        return dx, dwg, dwu, dwd

    rows, cols = P(("dp", "tp"), None), P("dp", "tp")
    weight, down = P(None, "tp"), P("tp", None)
    return jax.shard_map(
        step,
        mesh=mesh,
        in_specs=(rows, rows, cols, cols, weight, weight, down),
        out_specs=(rows, cols, cols, rows),
        check_vma=False,
    )
```
